32 devices in a mesh: wide: 16 (over z, y, x), narrow: 2 (over core).
Axes of the slice: x: 2, y: 2, z: 4, core: 2. Of those that a mesh axis runs over, the one named last changes fastest.
Arguments:
- features: bfloat16 [512, 16384], P('wide', 'narrow'), may hold values from -6 to 6
- queries: bfloat16 [1024, 16384], P('wide', 'narrow'), may hold values from -6 to 6
- damping: float32 [16384], P('wide'), may hold values from 0.25 to 4
Outputs:
- kernel: float32 [16384, 16384], P('wide', 'narrow')
- factor: float32 [16384, 256], P('wide')
- scores: float32 [1024, 512], P('wide', 'narrow')
The draws below stay inside these ranges and needn't reach their ends.
All inputs are finite; a program needn't handle non-finite values.
Results may differ from the reference program's by a relative error of at most 0.0003.
Values may be sent and summed in bfloat16 or wider, within the bound.
No kernel may reach another device: no remote copies, remote signals or barrier semaphores. Data moves between devices by JAX's collectives and lax.ppermute only.
A program may use at most 128 MiB of HBM per device.

```python
import math
import jax
import jax.numpy as jnp
from jax import lax

P_SIZE = 16384
PANEL = 128
PANELS = 2
SLAB = 512
QUERIES = 1024


def level_of(own_key, shape, split, low, top_value):
    def one(position, parts):
        heights = jax.random.uniform(jax.random.fold_in(jax.random.fold_in(own_key, 6), position), (parts,), jnp.float32, low / len(split), top_value / len(split))
        return jnp.repeat(jnp.exp(heights), shape[position] // parts).reshape((-1,) + (1,) * (len(shape) - position - 1))

    loudness = one(*split[0])
    for cut in split[1:]:
        loudness = loudness * one(*cut)
    return loudness


def noise(own_key, dims, deviation, most, cuts=(), kind=jnp.bfloat16):
    factor_of = level_of(own_key, dims, cuts, -0.22, 0.18) if cuts else 1.0
    entries = jax.random.normal(own_key, dims, jnp.float32) * deviation * factor_of
    return jnp.minimum(jnp.maximum(entries, -most), most).astype(kind)


def setup_inputs(seed: int = 0) -> dict:
    streams_of = jax.random.split(jax.random.key(seed), 4)
    features = noise(streams_of[0], (SLAB, P_SIZE), 1.0, 6.0, ((0, 16), (1, 2)))
    queries = noise(streams_of[1], (QUERIES, P_SIZE), 1.0, 6.0, ((0, 16), (1, 2)))
    damping = jnp.clip(jnp.exp(math.log(4.0) - 2.7725887 * jax.random.uniform(streams_of[2], (P_SIZE,), jnp.float32) ** level_of(streams_of[2], (P_SIZE,), ((0, 16),), -0.2, 0.2)), 0.25, 4.0)
    return dict(features=features, queries=queries, damping=damping)


def reference(features, queries, damping):
    products = lax.dot_general(features.astype(jnp.float32), features.astype(jnp.float32), (((0,), (0,)), ((), ())), preferred_element_type=jnp.float32)
    index_all = jnp.arange(P_SIZE, dtype=jnp.int32)
    kernel = products / SLAB
    kernel = kernel.at[index_all, index_all].add(damping)
    factors = []
    for panel_index in range(PANELS):
        offset = panel_index * PANEL
        pivot_block = kernel[offset:offset + PANEL, offset:offset + PANEL]
        pivot_factor = jnp.linalg.cholesky(pivot_block)
        columns = kernel[:, offset:offset + PANEL]
        lower_rows = lax.linalg.triangular_solve(pivot_factor, columns, left_side=False, lower=True, transpose_a=True)
        kernel = kernel - jnp.dot(lower_rows.astype(jnp.float32), lower_rows.T.astype(jnp.float32), precision=lax.Precision.HIGHEST, preferred_element_type=jnp.float32)
        finished = index_all < offset + PANEL
        kernel = jnp.where(finished[:, None] | finished[None, :], jnp.zeros_like(kernel), kernel)
        factors.append(lower_rows)
    scores = lax.dot_general(queries.astype(jnp.float32), features.astype(jnp.float32), (((1,), (1,)), ((), ())), preferred_element_type=jnp.float32)
    scores = scores * (1.0 / math.sqrt(P_SIZE))
    return (kernel, jnp.concatenate(factors, axis=1), scores)
```

```python
import math

import jax
import jax.numpy as jnp
from jax import lax
from jax.experimental import pallas as pl
from jax.experimental.pallas import tpu as pltpu
from jax.sharding import PartitionSpec as P


PANEL = 128
PANELS = 2
PIVOTS = PANEL * PANELS
TILE = 512
SLOTS = 4
HIGHEST = lax.Precision.HIGHEST


def dot(a, b, ca, cb, precision=None):
    return lax.dot_general(
        a, b, (((ca,), (cb,)), ((), ())), precision=precision, preferred_element_type=jnp.float32
    )


def split_bf16(value, parts):
    pieces = []
    for _ in range(parts):
        piece = lax.reduce_precision(value, 8, 7)
        pieces.append(piece.astype(jnp.bfloat16))
        value = value - piece
    return pieces


def inverse_factor(block, a_s, w_s):
    n = block.shape[0]
    sub = lax.broadcasted_iota(jnp.int32, (n, n), 0)
    lane = lax.broadcasted_iota(jnp.int32, (n, n), 1)
    lane8 = lax.broadcasted_iota(jnp.int32, (8, n), 1)
    sub8 = lax.broadcasted_iota(jnp.int32, (8, 1), 0)
    sub_col = lax.broadcasted_iota(jnp.int32, (n, 1), 0)
    a_s[...] = block
    w_s[...] = jnp.where(sub == lane, 1.0, 0.0)

    def step(b, carry):
        k0 = pl.multiple_of(b * 8, 8)
        rows = a_s[pl.ds(k0, 8), :]
        wrows = w_s[pl.ds(k0, 8), :]
        a = a_s[...]
        heads = [jnp.sum(jnp.where(lane8 == k0 + j, rows, 0.0), axis=1, keepdims=True) for j in range(8)]
        columns = [jnp.sum(jnp.where(lane == k0 + j, a, 0.0), axis=1, keepdims=True) for j in range(8)]
        scaled = []
        for j in range(8):
            inv = 1.0 / heads[j][j : j + 1, :]
            times = jnp.where(sub8 > j, heads[j], 0.0) * inv
            for m in range(j + 1, 8):
                entry = heads[m][j : j + 1, :]
                columns[m] = columns[m] - columns[j] * (entry * inv)
                heads[m] = heads[m] - times * entry
            scaled.append((rows[j : j + 1, :] * inv, wrows[j : j + 1, :] * inv))
            rows = rows - times * rows[j : j + 1, :]
            wrows = wrows - times * wrows[j : j + 1, :]
        w = w_s[...]
        for j in range(8):
            column = jnp.where(sub_col > k0 + 7, columns[j], 0.0)
            a = a - column * scaled[j][0]
            w = w - column * scaled[j][1]
        a_s[...] = a
        w_s[...] = w
        a_s[pl.ds(k0, 8), :] = rows
        w_s[pl.ds(k0, 8), :] = wrows
        return carry

    lax.fori_loop(0, n // 8, step, 0)
    diagonal = jnp.sum(jnp.where(sub == lane, a_s[...], 0.0), axis=1, keepdims=True)
    return w_s[...] * (1.0 / jnp.sqrt(diagonal))


def first_panel_body(slab, each, place_ref, packed_ref, other_ref, fp_ref, inv_ref, left_ref, rest_ref, a_s, w_s):
    mine = place_ref[1] == 0
    fp = jnp.where(mine, packed_ref[:, :each, :], other_ref[:, :each, :]).reshape(slab, PIVOTS)
    fp_ref[...] = fp
    tail = pl.ds(each, 16)
    tail = jnp.where(mine, packed_ref[place_ref[0], tail, :], other_ref[place_ref[0], tail, :])
    tail = tail.astype(jnp.float32)
    damping = tail[0:1, :] + tail[1:2, :] + tail[2:3, :]
    sub = lax.broadcasted_iota(jnp.int32, (PIVOTS, PIVOTS), 0)
    lane = lax.broadcasted_iota(jnp.int32, (PIVOTS, PIVOTS), 1)
    pivots = dot(fp, fp, 0, 0) / slab + jnp.where(sub == lane, damping, 0.0)
    inv = inverse_factor(pivots[:PANEL, :PANEL], a_s, w_s)
    left = dot(pivots[PANEL:, :PANEL], inv, 1, 1, HIGHEST)
    inv_ref[...] = inv
    left_ref[...] = left
    rest_ref[...] = pivots[PANEL:, PANEL:] - dot(left, left, 1, 1, HIGHEST)


def first_panel(place, packed, other, slab, each):
    f32 = jax.ShapeDtypeStruct((PANEL, PANEL), jnp.float32)
    return pl.pallas_call(
        lambda *refs: first_panel_body(slab, each, *refs),
        in_specs=[pl.BlockSpec(memory_space=pltpu.SMEM), pl.BlockSpec(memory_space=pltpu.VMEM)]
        + [pl.BlockSpec(memory_space=pltpu.VMEM)],
        out_shape=(jax.ShapeDtypeStruct((slab, PIVOTS), jnp.bfloat16), f32, f32, f32),
        scratch_shapes=[pltpu.VMEM((PANEL, PANEL), jnp.float32)] * 2,
        name="first_panel",
    )(place, packed, other)


def second_panel_body(inv_ref, left_ref, rest_ref, fp_ref, full_ref, middle_ref, a_s, w_s):
    slab = fp_ref.shape[0]
    first = inv_ref[...]
    inv = inverse_factor(rest_ref[...], a_s, w_s)
    below = -dot(dot(inv, left_ref[...], 1, 0, HIGHEST), first, 1, 0, HIGHEST)
    top = jnp.concatenate([first, jnp.zeros((PANEL, PANEL), jnp.float32)], axis=1)
    full = jnp.concatenate([top, jnp.concatenate([below, inv], axis=1)], axis=0)
    full_ref[...] = full
    basis = dot(full, fp_ref[...].astype(jnp.float32), 1, 1, HIGHEST)
    sub = lax.broadcasted_iota(jnp.int32, (slab, slab), 0)
    lane = lax.broadcasted_iota(jnp.int32, (slab, slab), 1)
    middle = jnp.where(sub == lane, 1.0, 0.0) - dot(basis, basis, 0, 0, HIGHEST) / slab
    for part in range(3):
        piece = middle.astype(jnp.bfloat16)
        middle_ref[part] = piece
        middle = middle - piece.astype(jnp.float32)


def second_panel(inv, left, rest, fp):
    slab = fp.shape[0]
    parts = jax.ShapeDtypeStruct((3, slab, slab), jnp.bfloat16)
    return pl.pallas_call(
        second_panel_body,
        out_shape=(jax.ShapeDtypeStruct((PIVOTS, PIVOTS), jnp.float32), parts),
        scratch_shapes=[pltpu.VMEM((PANEL, PANEL), jnp.float32)] * 2,
        name="second_panel",
    )(inv, left, rest, fp)


def group_scan_body(home_ref, queries_ref, own_ref, x_ref, y_ref, a_ref, b_ref, partial_ref, rows_ref):
    rows_here = rows_ref.shape[1]
    halves = a_ref.shape[1] // rows_here
    columns = [own_ref[...], x_ref[...], y_ref[...], jnp.concatenate([a_ref[...], b_ref[...]], axis=1)]
    partial_ref[...] = dot(jnp.concatenate(columns, axis=0), queries_ref[...], 1, 1)
    home = home_ref[0]
    at = pl.ds(pl.multiple_of(home * rows_here, 128), rows_here)
    early = pl.ds(pl.multiple_of(jnp.minimum(home, halves - 1) * rows_here, 128), rows_here)
    late = pl.ds(pl.multiple_of(jnp.maximum(home - halves, 0) * rows_here, 128), rows_here)
    diag = jnp.where(home < halves, a_ref[:, early], b_ref[:, late])
    rows_ref[...] = jnp.concatenate([own_ref[:, at], x_ref[:, at], y_ref[:, at], diag], axis=0)


def group_scan(home, queries, group, rows_here):
    each = group[0].shape[0]
    return pl.pallas_call(
        group_scan_body,
        in_specs=[pl.BlockSpec(memory_space=pltpu.SMEM)] + [pl.BlockSpec(memory_space=pltpu.VMEM)] * 6,
        out_shape=(
            jax.ShapeDtypeStruct((4 * each, queries.shape[0]), jnp.float32),
            jax.ShapeDtypeStruct((4 * each, rows_here), jnp.bfloat16),
        ),
        name="group_scan",
    )(home, queries, *group)


def row_sums(home, refs, at, fp_ref, middle_ref):
    rows = [jnp.where(home == 1, mine[...], other[...]) for mine, other in zip(*[iter(refs)] * 2)]
    rows = jnp.concatenate(rows, axis=0).T
    middle = jnp.concatenate([middle_ref[part, k] for part in range(3) for k in at], axis=0)
    front = jnp.concatenate([fp_ref[k] for k in at], axis=0)
    return dot(jnp.concatenate([rows] * 3, axis=1), middle, 1, 0), dot(rows, front, 1, 0)


def early_rows(home, groups, fp, middle, row_parts):
    size, rows_here = row_parts[0].shape
    slab = fp.shape[0]

    def body(home_ref, fp_ref, middle_ref, *refs):
        left, ahead = row_sums(home_ref[1], refs[:-2], groups, fp_ref, middle_ref)
        refs[-2][...] = left
        refs[-1][...] = ahead

    return pl.pallas_call(
        body,
        in_specs=[pl.BlockSpec(memory_space=pltpu.SMEM)]
        + [pl.BlockSpec(memory_space=pltpu.VMEM)] * (2 + len(row_parts)),
        out_shape=(
            jax.ShapeDtypeStruct((rows_here, slab), jnp.float32),
            jax.ShapeDtypeStruct((rows_here, PIVOTS), jnp.float32),
        ),
        name="early_rows",
    )(home, fp.reshape(-1, size, PIVOTS), middle.reshape(3, -1, size, slab), *row_parts)


def kernel_block_body(
    last, tile, ids_ref, damp_ref, early_ref, ahead_ref, fp_ref, inv_ref, middle_ref, mine_ref, other_ref, *refs
):
    out_ref, factor_ref, hi_s, lo_s, factor_s, slots, sems, factor_sem = refs[-8:]
    groups = list(zip(*[iter(refs[:-8])] * 5))
    rows, slab = hi_s.shape
    steps = out_ref.shape[1] // tile
    half_steps = steps // 2
    row0 = ids_ref[0]
    left, ahead = row_sums(ids_ref[2], [mine_ref, other_ref], [last], fp_ref, middle_ref)
    left = (left + early_ref[...]) / slab
    hi = left.astype(jnp.bfloat16)
    hi_s[...] = hi
    lo_s[...] = (left - hi.astype(jnp.float32)).astype(jnp.bfloat16)
    row_ids = row0 + lax.broadcasted_iota(jnp.int32, (rows, PIVOTS), 0)
    pivot_ids = lax.broadcasted_iota(jnp.int32, (rows, PIVOTS), 1)
    ahead = (ahead + ahead_ref[...]) / slab
    ahead = ahead + jnp.where(row_ids == pivot_ids, damp_ref[:, :PIVOTS], 0.0)
    factor_s[...] = dot(ahead, inv_ref[...], 1, 1, HIGHEST)
    factor_copy = pltpu.make_async_copy(factor_s, factor_ref, factor_sem)
    factor_copy.start()

    def store(step, slot):
        at = pl.ds(pl.multiple_of(step * tile, 128), tile)
        return pltpu.make_async_copy(slots.at[slot], out_ref.at[:, at], sems.at[slot])

    def one(step, carry):
        slot = lax.rem(step, SLOTS)
        col0 = ids_ref[1] + step * tile
        at = pl.ds(pl.multiple_of(step * tile, 128), tile)
        early = pl.ds(pl.multiple_of(jnp.minimum(step, half_steps - 1) * tile, 128), tile)
        late = pl.ds(pl.multiple_of(jnp.maximum(step - half_steps, 0) * tile, 128), tile)
        pieces = []
        for own, across_x, across_y, diag_a, diag_b in groups:
            diag = jnp.where(step < half_steps, diag_a[:, early], diag_b[:, late])
            pieces += [own[:, at], across_x[:, at], across_y[:, at], diag]
        columns = jnp.concatenate(pieces, axis=0)

        @pl.when(step >= SLOTS)
        def _():
            store(step - SLOTS, slot).wait()

        slots[slot] = dot(hi_s[...], columns, 1, 0) + dot(lo_s[...], columns, 1, 0)

        @pl.when((col0 < row0 + rows) & (row0 < col0 + tile))
        def _():
            row_ids = row0 + lax.broadcasted_iota(jnp.int32, (rows, tile), 0)
            col_ids = col0 + lax.broadcasted_iota(jnp.int32, (rows, tile), 1)
            own_at = pl.ds(pl.multiple_of(col0 - row0, 128), tile)
            slots[slot] = slots[slot] + jnp.where(row_ids == col_ids, damp_ref[:, own_at], 0.0)

        @pl.when(row0 < PIVOTS)
        def _():
            slots[slot, :PIVOTS, :] = jnp.zeros((PIVOTS, tile), jnp.float32)

        @pl.when(col0 < PIVOTS)
        def _():
            col_ids = col0 + lax.broadcasted_iota(jnp.int32, (1, tile), 1)
            slots[slot] = jnp.where(col_ids < PIVOTS, 0.0, slots[slot])

        store(step, slot).start()
        return carry

    lax.fori_loop(0, steps, one, 0)
    for step in range(max(0, steps - SLOTS), steps):
        store(step, step % SLOTS).wait()
    factor_copy.wait()


def kernel_block(ids, damping, early, fp, inverses, middle, last, rows_last, pieces):
    cols_here = pieces[0][0].shape[1]
    size, rows = rows_last[0].shape
    slab = fp.shape[0]
    tile = min(TILE, rows, cols_here // 2)
    fixed = [damping, *early, fp.reshape(-1, size, PIVOTS), inverses, middle.reshape(3, -1, size, slab), *rows_last]
    fixed += [piece for group in pieces for piece in group]
    return pl.pallas_call(
        lambda *refs: kernel_block_body(last, tile, *refs),
        in_specs=[pl.BlockSpec(memory_space=pltpu.SMEM)]
        + [pl.BlockSpec(memory_space=pltpu.VMEM)] * len(fixed),
        out_specs=(pl.BlockSpec(memory_space=pl.ANY), pl.BlockSpec(memory_space=pl.ANY)),
        out_shape=(
            jax.ShapeDtypeStruct((rows, cols_here), jnp.float32),
            jax.ShapeDtypeStruct((rows, PIVOTS), jnp.float32),
        ),
        scratch_shapes=[
            pltpu.VMEM((rows, slab), jnp.bfloat16),
            pltpu.VMEM((rows, slab), jnp.bfloat16),
            pltpu.VMEM((rows, PIVOTS), jnp.float32),
            pltpu.VMEM((SLOTS, rows, tile), jnp.float32),
            pltpu.SemaphoreType.DMA((SLOTS,)),
            pltpu.SemaphoreType.DMA,
        ],
        cost_estimate=pl.CostEstimate(
            flops=4 * rows * slab * cols_here,
            bytes_accessed=4 * rows * cols_here + 2 * slab * cols_here,
            transcendentals=0,
        ),
        name="kernel_block",
    )(ids, *fixed)


def solution(mesh):
    wide = mesh.shape["wide"]
    narrow = mesh.shape["narrow"]
    depth = wide // 4

    def index(x, y, z):
        return z * 4 + y * 2 + x

    spots = [(x, y, z) for z in range(depth) for y in range(2) for x in range(2)]
    swap_x = [(index(x, y, z), index(1 - x, y, z)) for x, y, z in spots]
    swap_y = [(index(x, y, z), index(x, 1 - y, z)) for x, y, z in spots]

    def shift(s):
        return [(index(x, y, z), index(x, y, (z + s) % depth)) for x, y, z in spots]

    def send(value, moves):
        return lax.ppermute(value, "wide", moves)

    def from_other(value, root):
        if narrow == 2:
            return lax.ppermute(value, "narrow", [(0, 1), (1, 0)])
        mine = lax.axis_index("narrow") == root
        return lax.psum(jnp.where(mine, value, jnp.zeros_like(value)), "narrow")

    sequence = []
    for r in range(1, depth // 2 + 1):
        sequence += [r] if depth - r == r else [r, depth - r]
    last = sequence[-1]

    def on_device(features, queries, damping):
        each, cols_here = features.shape
        rows_here = damping.shape[0]
        slab = each * wide
        half = cols_here // 2
        w = lax.axis_index("wide")
        n = lax.axis_index("narrow")

        damp_parts = jnp.stack(split_bf16(damping[:PIVOTS], 3))
        packed = jnp.concatenate(
            [features[:, :PIVOTS], damp_parts, jnp.zeros((13, PIVOTS), jnp.bfloat16)], axis=0
        )
        packed = jnp.stack([packed, send(packed, swap_x)])
        packed = jnp.concatenate([packed, send(packed, swap_y)], axis=0)
        packed = jnp.stack([packed] + [send(packed, shift(r)) for r in range(1, depth)])
        other = from_other(packed, 0).reshape(wide, each + 16, PIVOTS)
        packed = packed.reshape(wide, each + 16, PIVOTS)
        x, y, z = w % 2, (w // 2) % 2, w // 4
        place = jnp.stack([z * 4 + y * 2 + x, n]).astype(jnp.int32)
        fp, inv, left, rest = first_panel(place, packed, other, slab, each)
        inverses, middle = second_panel(inv, left, rest, fp)

        pieces = [None] * depth
        layers = {0: features}
        for r in [0] + sequence:
            if r and r <= depth // 2:
                layers[r] = send(layers[r - 1], shift(1))
            elif r:
                layers[r] = send(layers[(r + 1) % depth], shift(-1))
            layer = layers[r]
            across_x = send(layer, swap_x)
            across_y = send(layer, swap_y)
            diag_a = send(across_y[:, :half], swap_x)
            diag_b = send(across_x[:, half:], swap_y)
            pieces[r] = (layer, across_x, across_y, diag_a, diag_b)

        home = (w * rows_here) // cols_here
        begin = (w * rows_here) % cols_here // rows_here
        here = jnp.stack([begin, home == n]).astype(jnp.int32)
        row_parts = []
        partial = []
        for r in range(depth):
            part, rows = group_scan(here, queries, pieces[r], rows_here)
            row_parts.append((rows, from_other(rows, home)))
            partial.append(part)
        before = [r for r in range(depth) if r != last]
        early = early_rows(here, before, fp, middle, [rows for r in before for rows in row_parts[r]])

        partial = jnp.concatenate(partial, axis=0)
        spot = lax.broadcasted_iota(jnp.int32, (slab, 1), 0)
        group_id = spot // (4 * each)
        local = (spot // each) % 4
        example = (
            ((z - group_id) % depth) * 4 + (y ^ (local // 2)) * 2 + (x ^ (local % 2))
        ) * each + spot % each
        names = lax.broadcasted_iota(jnp.int32, (1, slab), 1)
        partial = dot(partial, (example == names).astype(jnp.float32), 0, 0, HIGHEST)
        scale = 1.0 / math.sqrt(cols_here * narrow)
        if narrow == 2:
            width = slab // 2
            keep = lax.dynamic_slice_in_dim(partial, n * width, width, axis=1)
            give = lax.dynamic_slice_in_dim(partial, (1 - n) * width, width, axis=1)
            other = lax.ppermute(give, "narrow", [(0, 1), (1, 0)])
            scores = (keep + other) * scale
        else:
            scores = lax.psum_scatter(partial, "narrow", scatter_dimension=1, tiled=True) * scale

        ids = jnp.stack([w * rows_here, n * cols_here, home == n]).astype(jnp.int32)
        kernel, factor = kernel_block(ids, damping[None, :], early, fp, inverses, middle, last, row_parts[last], pieces)
        return kernel, factor, scores

    return jax.shard_map(
        on_device,
        mesh=mesh,
        in_specs=(P("wide", "narrow"), P("wide", "narrow"), P("wide")),
        out_specs=(P("wide", "narrow"), P("wide", None), P("wide", "narrow")),
        check_vma=False,
    )
```

```python
import math

import jax
import jax.numpy as jnp
from jax import lax
from jax.experimental import pallas as pl
from jax.experimental.pallas import tpu as pltpu
from jax.sharding import PartitionSpec as P


PANEL = 128
PANELS = 2
PIVOTS = PANEL * PANELS
TILE = 512
SLOTS = 4
HIGHEST = lax.Precision.HIGHEST


def dot(a, b, ca, cb, precision=None):
    return lax.dot_general(
        a, b, (((ca,), (cb,)), ((), ())), precision=precision, preferred_element_type=jnp.float32
    )


def split_bf16(value, parts):
    pieces = []
    for _ in range(parts):
        piece = lax.reduce_precision(value, 8, 7)
        pieces.append(piece.astype(jnp.bfloat16))
        value = value - piece
    return pieces


def inverse_factor(block, a_s, w_s):
    n = block.shape[0]
    sub = lax.broadcasted_iota(jnp.int32, (n, n), 0)
    lane = lax.broadcasted_iota(jnp.int32, (n, n), 1)
    lane8 = lax.broadcasted_iota(jnp.int32, (8, n), 1)
    sub8 = lax.broadcasted_iota(jnp.int32, (8, 1), 0)
    sub_col = lax.broadcasted_iota(jnp.int32, (n, 1), 0)
    a_s[...] = block
    w_s[...] = jnp.where(sub == lane, 1.0, 0.0)

    def step(b, carry):
        k0 = pl.multiple_of(b * 8, 8)
        rows = a_s[pl.ds(k0, 8), :]
        wrows = w_s[pl.ds(k0, 8), :]
        a = a_s[...]
        heads = [jnp.sum(jnp.where(lane8 == k0 + j, rows, 0.0), axis=1, keepdims=True) for j in range(8)]
        columns = [jnp.sum(jnp.where(lane == k0 + j, a, 0.0), axis=1, keepdims=True) for j in range(8)]
        scaled = []
        for j in range(8):
            inv = 1.0 / heads[j][j : j + 1, :]
            times = jnp.where(sub8 > j, heads[j], 0.0) * inv
            for m in range(j + 1, 8):
                entry = heads[m][j : j + 1, :]
                columns[m] = columns[m] - columns[j] * (entry * inv)
                heads[m] = heads[m] - times * entry
            scaled.append((rows[j : j + 1, :] * inv, wrows[j : j + 1, :] * inv))
            rows = rows - times * rows[j : j + 1, :]
            wrows = wrows - times * wrows[j : j + 1, :]
        w = w_s[...]
        for j in range(8):
            column = jnp.where(sub_col > k0 + 7, columns[j], 0.0)
            a = a - column * scaled[j][0]
            w = w - column * scaled[j][1]
        a_s[...] = a
        w_s[...] = w
        a_s[pl.ds(k0, 8), :] = rows
        w_s[pl.ds(k0, 8), :] = wrows
        return carry

    lax.fori_loop(0, n // 8, step, 0)
    diagonal = jnp.sum(jnp.where(sub == lane, a_s[...], 0.0), axis=1, keepdims=True)
    return w_s[...] * (1.0 / jnp.sqrt(diagonal))


def first_panel_body(slab, each, place_ref, packed_ref, other_ref, fp_ref, inv_ref, left_ref, rest_ref, a_s, w_s):
    mine = place_ref[1] == 0
    fp = jnp.where(mine, packed_ref[:, :each, :], other_ref[:, :each, :]).reshape(slab, PIVOTS)
    fp_ref[...] = fp
    tail = pl.ds(each, 16)
    tail = jnp.where(mine, packed_ref[place_ref[0], tail, :], other_ref[place_ref[0], tail, :])
    tail = tail.astype(jnp.float32)
    damping = tail[0:1, :] + tail[1:2, :] + tail[2:3, :]
    sub = lax.broadcasted_iota(jnp.int32, (PIVOTS, PIVOTS), 0)
    lane = lax.broadcasted_iota(jnp.int32, (PIVOTS, PIVOTS), 1)
    pivots = dot(fp, fp, 0, 0) / slab + jnp.where(sub == lane, damping, 0.0)
    inv = inverse_factor(pivots[:PANEL, :PANEL], a_s, w_s)
    left = dot(pivots[PANEL:, :PANEL], inv, 1, 1, HIGHEST)
    inv_ref[...] = inv
    left_ref[...] = left
    rest_ref[...] = pivots[PANEL:, PANEL:] - dot(left, left, 1, 1, HIGHEST)


def first_panel(place, packed, other, slab, each):
    f32 = jax.ShapeDtypeStruct((PANEL, PANEL), jnp.float32)
    return pl.pallas_call(
        lambda *refs: first_panel_body(slab, each, *refs),
        in_specs=[pl.BlockSpec(memory_space=pltpu.SMEM), pl.BlockSpec(memory_space=pltpu.VMEM)]
        + [pl.BlockSpec(memory_space=pltpu.VMEM)],
        out_shape=(jax.ShapeDtypeStruct((slab, PIVOTS), jnp.bfloat16), f32, f32, f32),
        scratch_shapes=[pltpu.VMEM((PANEL, PANEL), jnp.float32)] * 2,
        name="first_panel",
    )(place, packed, other)


def second_panel_body(damp_ref, inv_ref, left_ref, rest_ref, fp_ref, pivot_ref, factors_ref, a_s, w_s):
    slab = fp_ref.shape[0]
    first = inv_ref[...]
    inv = inverse_factor(rest_ref[...], a_s, w_s)
    below = -dot(dot(inv, left_ref[...], 1, 0, HIGHEST), first, 1, 0, HIGHEST)
    top = jnp.concatenate([first, jnp.zeros((PANEL, PANEL), jnp.float32)], axis=1)
    full = jnp.concatenate([top, jnp.concatenate([below, inv], axis=1)], axis=0)
    pivot_ref[...] = (full * damp_ref[:, :PIVOTS]).T
    basis = dot(fp_ref[...].astype(jnp.float32), full, 1, 1, HIGHEST)
    sub = lax.broadcasted_iota(jnp.int32, (slab, slab), 0)
    lane = lax.broadcasted_iota(jnp.int32, (slab, slab), 1)
    middle = jnp.where(sub == lane, 1.0, 0.0) - dot(basis, basis, 1, 1, HIGHEST) / slab
    factors = jnp.concatenate([middle, basis], axis=1)
    for part in range(3):
        piece = factors.astype(jnp.bfloat16)
        factors_ref[part] = piece
        factors = factors - piece.astype(jnp.float32)


def second_panel(damping, inv, left, rest, fp):
    slab = fp.shape[0]
    return pl.pallas_call(
        second_panel_body,
        out_shape=(
            jax.ShapeDtypeStruct((PIVOTS, PIVOTS), jnp.float32),
            jax.ShapeDtypeStruct((3, slab, slab + PIVOTS), jnp.bfloat16),
        ),
        scratch_shapes=[pltpu.VMEM((PANEL, PANEL), jnp.float32)] * 2,
        name="second_panel",
    )(damping, inv, left, rest, fp)


def own_rows_body(home_ref, *refs):
    pieces, rows_ref, sems = refs[:-2], refs[-2], refs[-1]
    rows_here = rows_ref.shape[1]
    at = pl.ds(pl.multiple_of(home_ref[0] * rows_here, 128), rows_here)
    copies = []
    begin = 0
    for k, piece in enumerate(pieces):
        size = piece.shape[0]
        copies.append(pltpu.make_async_copy(piece.at[:, at], rows_ref.at[pl.ds(begin, size), :], sems.at[k]))
        copies[-1].start()
        begin += size
    for copy in copies:
        copy.wait()


def own_rows(home, group, rows_here):
    size = sum(piece.shape[0] for piece in group)
    return pl.pallas_call(
        own_rows_body,
        in_specs=[pl.BlockSpec(memory_space=pltpu.SMEM)] + [pl.BlockSpec(memory_space=pl.ANY)] * len(group),
        out_specs=pl.BlockSpec(memory_space=pltpu.VMEM),
        out_shape=jax.ShapeDtypeStruct((size, rows_here), jnp.bfloat16),
        scratch_shapes=[pltpu.SemaphoreType.DMA((len(group),))],
        name="own_rows",
    )(home, *group)


def row_sums(home, refs, factors):
    rows = [jnp.where(home == 1, mine[...], other[...]) for mine, other in zip(*[iter(refs)] * 2)]
    rows = jnp.concatenate(rows, axis=0).T
    return dot(jnp.concatenate([rows] * 3, axis=1), jnp.concatenate(factors, axis=0), 1, 0)


def early_rows(home, at, factors, row_parts):
    rows_here = row_parts[0].shape[1]

    def body(home_ref, factors_ref, *refs):
        chosen = [factors_ref[part, a:b] for part in range(3) for a, b in at]
        refs[-1][...] = row_sums(home_ref[1], refs[:-1], chosen)

    return pl.pallas_call(
        body,
        in_specs=[pl.BlockSpec(memory_space=pltpu.SMEM)]
        + [pl.BlockSpec(memory_space=pltpu.VMEM)] * (1 + len(row_parts)),
        out_shape=jax.ShapeDtypeStruct((rows_here, factors.shape[2]), jnp.float32),
        name="early_rows",
    )(home, factors, *row_parts)


def kernel_block_body(
    at, sizes, tile, ids_ref, damp_ref, pivot_ref, early_any, factors_any, queries_any, *refs
):
    out_ref, factor_ref, scores_ref, hi_s, lo_s, factor_s, columns_s = refs[-15:-8]
    early_ref, factors_ref, queries_ref, first_sems, slots, sems, factor_sem, load_sems = refs[-8:]
    parts, pieces = refs[: 2 * len(at)], refs[2 * len(at) : -15]
    needs = [pair for entry in at for pair in entry]
    firsts = []
    spot = 0
    for a, b in needs:
        for part in range(3):
            firsts.append((factors_any.at[part, pl.ds(a, b - a)], factors_ref.at[part, pl.ds(spot, b - a)]))
        spot += b - a
    firsts += [(early_any, early_ref), (queries_any, queries_ref)]
    firsts = [pltpu.make_async_copy(*pair, first_sems.at[k]) for k, pair in enumerate(firsts)]
    for copy in firsts:
        copy.start()
    rows, slab = hi_s.shape
    cols_here = out_ref.shape[1]
    steps = cols_here // tile
    loads = []
    begin = 0
    for k, piece in enumerate(pieces):
        size, width = piece.shape
        place = columns_s.at[pl.ds(begin, size), :]
        if sizes[k]:
            offset = ids_ref[5] if sizes[k] == 1 else (cols_here - width) - ids_ref[5]
            place = columns_s.at[pl.ds(begin, size), pl.ds(pl.multiple_of(offset, 128), width)]
        loads.append(pltpu.make_async_copy(piece, place, load_sems.at[k]))
        loads[-1].start()
        begin += size if sizes[k] != 1 else 0
    row0 = ids_ref[0]
    for copy in firsts[:-2]:
        copy.wait()
    sums = row_sums(ids_ref[2], parts, [factors_ref[part] for part in range(3)])
    for copy in firsts[-2:]:
        copy.wait()
    sums = (sums + early_ref[...]) / slab
    left = sums[:, :slab]
    hi = left.astype(jnp.bfloat16)
    hi_s[...] = hi
    lo_s[...] = (left - hi.astype(jnp.float32)).astype(jnp.bfloat16)
    factor_s[...] = sums[:, slab:]

    @pl.when(row0 < PIVOTS)
    def _():
        factor_s[:PIVOTS, :] = factor_s[:PIVOTS, :] + pivot_ref[...]

    factor_copy = pltpu.make_async_copy(factor_s, factor_ref, factor_sem)
    factor_copy.start()

    def store(step, slot):
        at = pl.ds(pl.multiple_of(step * tile, 128), tile)
        return pltpu.make_async_copy(slots.at[slot], out_ref.at[:, at], sems.at[slot])

    def one(step, carry):
        slot = lax.rem(step, SLOTS)
        col0 = ids_ref[1] + step * tile
        at = pl.ds(pl.multiple_of(step * tile, 128), tile)
        columns = columns_s[:, at]

        @pl.when(step >= SLOTS)
        def _():
            store(step - SLOTS, slot).wait()

        slots[slot] = dot(hi_s[...], columns, 1, 0) + dot(lo_s[...], columns, 1, 0)

        @pl.when((col0 < row0 + rows) & (row0 < col0 + tile))
        def _():
            row_ids = row0 + lax.broadcasted_iota(jnp.int32, (rows, tile), 0)
            col_ids = col0 + lax.broadcasted_iota(jnp.int32, (rows, tile), 1)
            own_at = pl.ds(pl.multiple_of(col0 - row0, 128), tile)
            slots[slot] = slots[slot] + jnp.where(row_ids == col_ids, damp_ref[:, own_at], 0.0)

        @pl.when(row0 < PIVOTS)
        def _():
            slots[slot, :PIVOTS, :] = jnp.zeros((PIVOTS, tile), jnp.float32)

        @pl.when(col0 < PIVOTS)
        def _():
            col_ids = col0 + lax.broadcasted_iota(jnp.int32, (1, tile), 1)
            slots[slot] = jnp.where(col_ids < PIVOTS, 0.0, slots[slot])

        store(step, slot).start()
        return carry

    for load in loads:
        load.wait()
    lax.fori_loop(0, steps, one, 0)

    partial = dot(queries_ref[...], columns_s[...], 1, 1)
    each = pieces[0].shape[0]
    depth = slab // (4 * each)
    wide = row0 // rows
    x, y, z = lax.rem(wide, 2), lax.rem(wide // 2, 2), wide // 4
    width = scores_ref.shape[2]
    spot = lax.broadcasted_iota(jnp.int32, (slab, width), 0)
    name = lax.broadcasted_iota(jnp.int32, (slab, width), 1)
    block = spot // each
    local = lax.rem(block, 4)
    plane = lax.rem(z - block // 4 + depth, depth)
    example = (plane * 4 + (y ^ (local // 2)) * 2 + (x ^ lax.rem(local, 2))) * each + lax.rem(spot, each)
    for part in range(2):
        chosen = jnp.where(example == name + ids_ref[3 + part], 1.0, 0.0)
        scores_ref[part] = dot(partial, chosen, 1, 0, HIGHEST)
    for step in range(max(0, steps - SLOTS), steps):
        store(step, step % SLOTS).wait()
    factor_copy.wait()


def kernel_block(ids, damping, early, pivot_term, factors, queries, at, row_parts, pieces, sizes):
    cols_here = pieces[0].shape[1]
    rows = row_parts[0].shape[1]
    slab = factors.shape[1]
    count = queries.shape[0]
    tile = min(TILE, rows, cols_here // 2)
    fixed = [damping, pivot_term]
    loose = [early, factors, queries]
    needs = [b - a for entry in at for a, b in entry]
    return pl.pallas_call(
        lambda *refs: kernel_block_body(at, sizes, tile, *refs),
        in_specs=[pl.BlockSpec(memory_space=pltpu.SMEM)]
        + [pl.BlockSpec(memory_space=pltpu.VMEM)] * len(fixed)
        + [pl.BlockSpec(memory_space=pl.ANY)] * len(loose)
        + [pl.BlockSpec(memory_space=pltpu.VMEM)] * len(row_parts)
        + [pl.BlockSpec(memory_space=pl.ANY)] * len(pieces),
        out_specs=(
            pl.BlockSpec(memory_space=pl.ANY),
            pl.BlockSpec(memory_space=pl.ANY),
            pl.BlockSpec(memory_space=pltpu.VMEM),
        ),
        out_shape=(
            jax.ShapeDtypeStruct((rows, cols_here), jnp.float32),
            jax.ShapeDtypeStruct((rows, PIVOTS), jnp.float32),
            jax.ShapeDtypeStruct((2, count, slab // 2), jnp.float32),
        ),
        scratch_shapes=[
            pltpu.VMEM((rows, slab), jnp.bfloat16),
            pltpu.VMEM((rows, slab), jnp.bfloat16),
            pltpu.VMEM((rows, PIVOTS), jnp.float32),
            pltpu.VMEM((slab, cols_here), jnp.bfloat16),
            pltpu.VMEM((rows, slab + PIVOTS), jnp.float32),
            pltpu.VMEM((3, sum(needs), slab + PIVOTS), jnp.bfloat16),
            pltpu.VMEM(queries.shape, jnp.bfloat16),
            pltpu.SemaphoreType.DMA((3 * len(needs) + 2,)),
            pltpu.VMEM((SLOTS, rows, tile), jnp.float32),
            pltpu.SemaphoreType.DMA((SLOTS,)),
            pltpu.SemaphoreType.DMA,
            pltpu.SemaphoreType.DMA((len(pieces),)),
        ],
        cost_estimate=pl.CostEstimate(
            flops=4 * rows * slab * cols_here,
            bytes_accessed=4 * rows * cols_here + 2 * slab * cols_here,
            transcendentals=0,
        ),
        name="kernel_block",
    )(ids, *fixed, *loose, *row_parts, *pieces)


def solution(mesh):
    wide = mesh.shape["wide"]
    narrow = mesh.shape["narrow"]
    depth = wide // 4

    def index(x, y, z):
        return z * 4 + y * 2 + x

    spots = [(x, y, z) for z in range(depth) for y in range(2) for x in range(2)]
    swap_x = [(index(x, y, z), index(1 - x, y, z)) for x, y, z in spots]
    swap_y = [(index(x, y, z), index(x, 1 - y, z)) for x, y, z in spots]

    def shift(s):
        return [(index(x, y, z), index(x, y, (z + s) % depth)) for x, y, z in spots]

    def send(value, moves):
        return lax.ppermute(value, "wide", moves)

    def from_other(value, root):
        if narrow == 2:
            return lax.ppermute(value, "narrow", [(0, 1), (1, 0)])
        mine = lax.axis_index("narrow") == root
        return lax.psum(jnp.where(mine, value, jnp.zeros_like(value)), "narrow")

    sequence = []
    for r in range(1, depth // 2 + 1):
        sequence += [r] if depth - r == r else [r, depth - r]

    def on_device(features, queries, damping):
        each, cols_here = features.shape
        rows_here = damping.shape[0]
        slab = each * wide
        w = lax.axis_index("wide")
        n = lax.axis_index("narrow")

        damp_parts = jnp.stack(split_bf16(damping[:PIVOTS], 3))
        packed = jnp.concatenate(
            [features[:, :PIVOTS], damp_parts, jnp.zeros((13, PIVOTS), jnp.bfloat16)], axis=0
        )
        packed = jnp.stack([packed, send(packed, swap_x)])
        packed = jnp.concatenate([packed, send(packed, swap_y)], axis=0)
        packed = jnp.stack([packed] + [send(packed, shift(r)) for r in range(1, depth)])
        other = from_other(packed, 0).reshape(wide, each + 16, PIVOTS)
        packed = packed.reshape(wide, each + 16, PIVOTS)
        x, y, z = w % 2, (w // 2) % 2, w // 4
        place = jnp.stack([z * 4 + y * 2 + x, n]).astype(jnp.int32)
        fp, inv, left, rest = first_panel(place, packed, other, slab, each)
        pivot_term, factors = second_panel(damping[None, :], inv, left, rest, fp)

        half = cols_here // 2
        begin = (w * rows_here) % cols_here // rows_here

        def home_half(place):
            return (place * rows_here) % cols_here // half * half

        layers = {0: features}
        direct = {}
        diagonal = {}
        turns = [0] + sequence
        for turn, r in enumerate(turns):
            if r and r <= depth // 2:
                layers[r] = send(layers[r - 1], shift(1))
            elif r:
                layers[r] = send(layers[(r + 1) % depth], shift(-1))
            across_x = send(layers[r], swap_x)
            across_y = send(layers[r], swap_y)
            direct[r] = [layers[r], across_x, across_y]
            source, moves, peer = (across_x, swap_y, w ^ 2) if turn % 2 else (across_y, swap_x, w ^ 1)
            if turn < depth - 2:
                diagonal[r] = [send(source, moves)]
                continue
            first = home_half(peer)
            near = lax.dynamic_slice_in_dim(source, first, half, axis=1)
            far = lax.dynamic_slice_in_dim(source, half - first, half, axis=1)
            diagonal[r] = [send(near, moves), send(far, moves)]

        home = (w * rows_here) // cols_here
        here = jnp.stack([begin, home == n]).astype(jnp.int32)
        parts = []
        at = []
        for some in (turns[:-1], turns[-1:]):
            group = [piece for r in some for piece in direct[r] + (diagonal[r] if r in turns[:-2] else [])]
            rows = own_rows(here, group, rows_here)
            parts.append((rows, from_other(rows, home)))
            at.append([(4 * each * r, 4 * each * r + (4 if r in turns[:-2] else 3) * each) for r in some])
        inside = begin * rows_here - home_half(w)
        late = [lax.dynamic_slice_in_dim(diagonal[r][0], inside, rows_here, axis=1) for r in turns[-2:]]
        late = jnp.concatenate(late, axis=0)
        late = (late, from_other(late, home))
        late_at = [(4 * each * r + 3 * each, 4 * each * (r + 1)) for r in turns[-2:]]
        early = early_rows(here, at[0], factors, parts[0])

        split = [n * (slab // 2), (1 - n) * (slab // 2)] if narrow == 2 else [0, slab // 2]
        ids = [w * rows_here, n * cols_here, home == n, *split, home_half(w)]
        ids = jnp.stack([jnp.asarray(i).astype(jnp.int32) for i in ids])
        columns = [piece for r in range(depth) for piece in direct[r] + diagonal[r]]
        sizes = [s for r in range(depth) for s in ([0] * 4 if r in turns[:-2] else [0, 0, 0, 1, 2])]
        kernel, factor, partial = kernel_block(
            ids,
            damping[None, :],
            early,
            pivot_term,
            factors,
            queries,
            [at[1], late_at],
            [*parts[1], *late],
            columns,
            sizes,
        )
        scale = 1.0 / math.sqrt(cols_here * narrow)
        if narrow == 2:
            other = lax.ppermute(partial[1], "narrow", [(0, 1), (1, 0)])
            scores = (partial[0] + other) * scale
        else:
            partial = jnp.concatenate([partial[0], partial[1]], axis=1)
            scores = lax.psum_scatter(partial, "narrow", scatter_dimension=1, tiled=True) * scale
        return kernel, factor, scores

    return jax.shard_map(
        on_device,
        mesh=mesh,
        in_specs=(P("wide", "narrow"), P("wide", "narrow"), P("wide")),
        out_specs=(P("wide", "narrow"), P("wide", None), P("wide", "narrow")),
        check_vma=False,
    )
```
